8 devices in a mesh: batch: 1 (over z), dap: 8 (over y, x, core).
Axes of the slice: x: 2, y: 2, z: 1, core: 2. Of those that a mesh axis runs over, the one named last changes fastest.
Arguments:
- pair: bfloat16 [512, 512, 128], P(('batch', 'dap'))
- pair_mask: int32 [512, 512], P(('batch', 'dap'))
- ln_in: bfloat16 [2, 2, 128], replicated
- w_proj: bfloat16 [2, 128, 512], replicated
- b_proj: bfloat16 [2, 512], replicated
- w_gate: bfloat16 [2, 128, 128], replicated
- b_gate: bfloat16 [2, 128], replicated
- ln_out: bfloat16 [2, 2, 128], replicated
- w_out: bfloat16 [2, 128, 128], replicated
- b_out: bfloat16 [2, 128], replicated
Outputs:
- output: bfloat16 [512, 512, 128], P(('batch', 'dap'))
All inputs are finite; a program needn't handle non-finite values.
Results may differ from the reference program's by a relative error of at most 0.00381369.
Values are sent between devices in bfloat16 or wider.
A program may use at most 1 GiB of HBM per device.

```python
import jax
import jax.numpy as jnp
from jax import lax

N = 512
CZ = 128
CH = 128
LN_EPS = 1e-5


def setup_inputs(seed: int = 0, part: int = 0) -> dict:
    base_key = jax.random.key(seed)
    part_key = jax.random.fold_in(base_key, part)
    pair_key, mask_key = jax.random.split(part_key)
    weight_keys = jax.random.split(jax.random.fold_in(base_key, 1000), 10)
    pair = jax.random.normal(pair_key, (N, N, CZ), jnp.float32)
    pair_mask = (jax.random.randint(mask_key, (N, N), 0, 8) > 0).astype(jnp.int32)
    ln_in = jnp.stack([1.0 + 0.3 * jax.random.normal(weight_keys[0], (2, CZ), jnp.float32),
                       0.3 * jax.random.normal(weight_keys[1], (2, CZ), jnp.float32)], axis=1)
    w_proj = jax.random.normal(weight_keys[2], (2, CZ, 4 * CH), jnp.float32) * CZ ** -0.5
    b_proj = 0.5 * jax.random.normal(weight_keys[3], (2, 4 * CH), jnp.float32)
    w_gate = jax.random.normal(weight_keys[4], (2, CZ, CZ), jnp.float32) * CZ ** -0.5
    b_gate = 0.5 * jax.random.normal(weight_keys[5], (2, CZ), jnp.float32)
    ln_out = jnp.stack([1.0 + 0.3 * jax.random.normal(weight_keys[6], (2, CH), jnp.float32),
                        0.3 * jax.random.normal(weight_keys[7], (2, CH), jnp.float32)], axis=1)
    w_out = jax.random.normal(weight_keys[8], (2, CH, CZ), jnp.float32) * CH ** -0.5
    b_out = 0.5 * jax.random.normal(weight_keys[9], (2, CZ), jnp.float32)
    return {
        "pair": pair.astype(jnp.bfloat16),
        "pair_mask": pair_mask,
        "ln_in": ln_in.astype(jnp.bfloat16),
        "w_proj": w_proj.astype(jnp.bfloat16),
        "b_proj": b_proj.astype(jnp.bfloat16),
        "w_gate": w_gate.astype(jnp.bfloat16),
        "b_gate": b_gate.astype(jnp.bfloat16),
        "ln_out": ln_out.astype(jnp.bfloat16),
        "w_out": w_out.astype(jnp.bfloat16),
        "b_out": b_out.astype(jnp.bfloat16),
    }


def layer_norm(values, scale, offset):
    centred = values - jnp.mean(values, axis=-1, keepdims=True)
    variance = jnp.mean(centred * centred, axis=-1, keepdims=True)
    return centred * lax.rsqrt(variance + LN_EPS) * scale.astype(jnp.float32) + offset.astype(jnp.float32)


def channel_product(left, right, contract_form):
    groups = CH // 16
    left_groups = jnp.moveaxis(left.reshape(N, N, groups, 16), 2, 0)
    right_groups = jnp.moveaxis(right.reshape(N, N, groups, 16), 2, 0)

    def group_sum(operands):
        return jnp.einsum(contract_form, operands[0].astype(jnp.float32), operands[1].astype(jnp.float32))

    summed = lax.map(group_sum, (left_groups, right_groups))
    return jnp.moveaxis(summed, 0, 2).reshape(N, N, CH)


def tri_layer(pair, keep_mask, ln_in, w_proj, b_proj, w_gate, b_gate, ln_out, w_out, b_out, contract_form):
    row_blocks = N // 8

    def make_sides(operands):
        block, mask_block = operands
        normed = layer_norm(block.astype(jnp.float32), ln_in[0], ln_in[1]).astype(jnp.bfloat16)
        projected = jnp.dot(normed.reshape(8 * N, CZ), w_proj, preferred_element_type=jnp.float32)
        projected = (projected + b_proj.astype(jnp.float32)).reshape(8, N, 4 * CH)
        left = mask_block * jax.nn.sigmoid(projected[..., CH:2 * CH]) * projected[..., :CH]
        right = mask_block * jax.nn.sigmoid(projected[..., 3 * CH:]) * projected[..., 2 * CH:3 * CH]
        return normed, left.astype(jnp.bfloat16), right.astype(jnp.bfloat16)

    pair_blocks = pair.reshape(row_blocks, 8, N, CZ)
    normed, left, right = lax.map(make_sides, (pair_blocks, keep_mask.reshape(row_blocks, 8, N, 1)))
    tri_sum = channel_product(left.reshape(N, N, CH), right.reshape(N, N, CH), contract_form)

    def finish(operands):
        block, normed_block, tri_block = operands
        tri_norm = layer_norm(tri_block, ln_out[0], ln_out[1]).astype(jnp.bfloat16)
        update = jnp.dot(tri_norm.reshape(8 * N, CH), w_out, preferred_element_type=jnp.float32) + b_out.astype(jnp.float32)
        gates = jax.nn.sigmoid(jnp.dot(normed_block.reshape(8 * N, CZ), w_gate, preferred_element_type=jnp.float32) + b_gate.astype(jnp.float32))
        return (block.astype(jnp.float32) + (gates * update).reshape(8, N, CZ)).astype(jnp.bfloat16)

    result = lax.map(finish, (pair_blocks, normed, tri_sum.reshape(row_blocks, 8, N, CH)))
    return result.reshape(N, N, CZ)


def reference(pair, pair_mask, ln_in, w_proj, b_proj, w_gate, b_gate, ln_out, w_out, b_out):
    keep_mask = pair_mask.astype(jnp.float32)[..., None]
    first = tri_layer(pair, keep_mask, ln_in[0], w_proj[0], b_proj[0], w_gate[0], b_gate[0],
                      ln_out[0], w_out[0], b_out[0], "ikc,jkc->ijc")
    return tri_layer(first, keep_mask, ln_in[1], w_proj[1], b_proj[1], w_gate[1], b_gate[1],
                     ln_out[1], w_out[1], b_out[1], "kic,kjc->ijc")
```

```python
import functools

import jax
import jax.numpy as jnp
from jax import lax
from jax.experimental import pallas as pl
from jax.experimental.pallas import tpu as pltpu
from jax.sharding import PartitionSpec as P

f32, bf16 = jnp.float32, jnp.bfloat16
LN_EPS = 1e-5
CH = 128
EXT = CH + 16
ROWS = 16
PITCH = 24
ROW_PITCH = 136
VMEM = 56 * 2**20


def norm_columns(x, scale, offset):
    mean = jnp.sum(x, axis=0, keepdims=True) * (1.0 / CH)
    centred = x - mean
    var = jnp.sum(centred * centred, axis=0, keepdims=True) * (1.0 / CH)
    return centred * lax.rsqrt(var + LN_EPS) * scale + offset


def extend(columns, row):
    n = columns.shape[1]
    first = lax.broadcasted_iota(jnp.int32, (16, n), 0) == 0
    extra = jnp.where(first, jnp.broadcast_to(row, (16, n)), 0.0).astype(bf16)
    return jnp.concatenate([columns, extra], axis=0)


def twice(ref):
    return jnp.concatenate([ref[...]] * 2, axis=1)


def store_gated(proj, store):
    for q in range(proj.shape[0] // 16):
        value, gate = proj[16 * q:16 * q + 8], proj[16 * q + 8:16 * q + 16]
        side = (jnp.tanh(gate) + 1.0) * value
        for t in range(2):
            store(q, t, side[:, 128 * t:128 * t + 128])


def project_body(z_ref, m_ref, w_ref, sc_ref, of_ref, a_ref, b_ref, zt_ref, znt_ref, scr):
    scale, offset = twice(sc_ref), twice(of_ref)

    def row(i, carry):
        zt = z_ref[i].T
        zt_ref[i] = zt
        zn = norm_columns(zt.astype(f32), scale, offset).astype(bf16)
        znt_ref[i] = zn
        m = m_ref[pl.ds(i, 1), :]
        proj = jnp.dot(w_ref[...], extend(zn * m.astype(bf16), m), preferred_element_type=f32)

        def store(q, t, tile):
            scr[t, pl.ds(8 * q * PITCH + i, 8, stride=PITCH), :] = tile

        store_gated(proj, store)
        return carry

    lax.fori_loop(0, ROWS, row, 0, unroll=8)
    for side, out in ((0, a_ref), (1, b_ref)):
        def channel(q, carry):
            for u in range(8):
                c = q * 8 + u
                start = pl.multiple_of((side * CH + c) * PITCH, 8)
                for t in range(2):
                    out[c, :, 128 * t:128 * t + 128] = scr[t, pl.ds(start, ROWS), :].astype(bf16)
            return carry

        lax.fori_loop(0, CH // 8, channel, 0)


def whole(*shape):
    return pl.BlockSpec(shape, lambda *ids: (0,) * len(shape))


def params(n=1):
    return pltpu.CompilerParams(dimension_semantics=("arbitrary",) * n, vmem_limit_bytes=VMEM)


def cost(flops, nbytes):
    return pl.CostEstimate(flops=flops, bytes_accessed=nbytes, transcendentals=0)


def project(z, m, w, scale, offset):
    rows, cols, _ = z.shape
    return pl.pallas_call(
        project_body,
        grid=(rows // ROWS, cols // 256),
        in_specs=[pl.BlockSpec((ROWS, 256, CH), lambda i, k: (i, k, 0)),
                  pl.BlockSpec((ROWS, 256), lambda i, k: (i, k)),
                  whole(4 * CH, EXT), whole(CH, CH), whole(CH, CH)],
        out_specs=[pl.BlockSpec((CH, ROWS, 256), lambda i, k: (0, i, k))] * 2
        + [pl.BlockSpec((ROWS, CH, 256), lambda i, k: (i, 0, k))] * 2,
        out_shape=[jax.ShapeDtypeStruct((CH, rows, cols), bf16)] * 2
        + [jax.ShapeDtypeStruct((rows, CH, cols), bf16)] * 2,
        scratch_shapes=[pltpu.VMEM((2, 2 * CH * PITCH, 128), f32)],
        compiler_params=params(2),
        cost_estimate=cost(rows * cols * 2**19, rows * cols * 1200),
        name="project",
    )(z, m, w, scale, offset)


def outgoing_body(n_left, n_right, h_ref, *refs):
    left = refs[:n_left]
    mine, theirs = refs[n_left:n_left + n_right], refs[n_left + n_right:n_left + 2 * n_right]
    o_ref, scr = refs[n_left + 2 * n_right:]
    at_mine, at_theirs = pl.multiple_of(64 * h_ref[0], 64), pl.multiple_of(64 - 64 * h_ref[0], 64)
    for c in range(o_ref.shape[0]):
        for s in range(n_right):
            scr[c, pl.ds(128 * s + at_mine, 64), :] = mine[s][c]
            scr[c, pl.ds(128 * s + at_theirs, 64), :] = theirs[s][c]
        a = jnp.concatenate([ref[c] for ref in left], axis=0)
        o_ref[c] = lax.dot_general(a, scr[c], (((1,), (1,)), ((), ())), preferred_element_type=f32)


def outgoing(h, left, mine, theirs):
    block = 4
    _, rows, cols = left[0].shape
    nl, nr = len(left), len(mine)
    side = pl.BlockSpec((block, rows, cols), lambda c: (c, 0, 0))
    return pl.pallas_call(
        functools.partial(outgoing_body, nl, nr),
        grid=(CH // block,),
        in_specs=[pl.BlockSpec(memory_space=pltpu.SMEM)] + [side] * (nl + 2 * nr),
        out_specs=pl.BlockSpec((block, nl * rows, nr * 2 * rows), lambda c: (c, 0, 0)),
        out_shape=jax.ShapeDtypeStruct((CH, nl * rows, nr * 2 * rows), f32),
        scratch_shapes=[pltpu.VMEM((block, nr * 2 * rows, cols), bf16)],
        compiler_params=params(),
        cost_estimate=cost(CH * nl * nr * rows * 2 * rows * cols * 4, CH * rows * (nl + 2 * nr) * cols * 4),
        name="outgoing",
    )(h, *left, *mine, *theirs)


def incoming_body(n_parts, h_ref, *refs):
    left, right = refs[:4], refs[4:4 + 4 * n_parts]
    keep_ref, send_ref, scr = refs[4 + 4 * n_parts:]
    at_mine, at_theirs = pl.multiple_of(64 * h_ref[0], 64), pl.multiple_of(64 - 64 * h_ref[0], 64)
    for c in range(keep_ref.shape[0]):
        a = jnp.concatenate([ref[c] for ref in left], axis=0)
        b = jnp.concatenate([jnp.concatenate([right[s * n_parts + p][c] for p in range(n_parts)], axis=1)
                             for s in range(4)], axis=0)
        scr[c] = lax.dot_general(a, b, (((0,), (0,)), ((), ())), preferred_element_type=f32)
        keep_ref[c] = scr[c, pl.ds(at_mine, 64), :]
        send_ref[c] = scr[c, pl.ds(at_theirs, 64), :]


def incoming(h, left, right):
    block = 4
    parts = [part for row in right for part in row]
    spec = lambda x: pl.BlockSpec((block,) + x.shape[1:], lambda c: (c, 0, 0))
    return pl.pallas_call(
        functools.partial(incoming_body, len(right[0])),
        grid=(CH // block,),
        in_specs=[pl.BlockSpec(memory_space=pltpu.SMEM)] + [spec(x) for x in left + parts],
        out_specs=[pl.BlockSpec((block, 64, 512), lambda c: (c, 0, 0))] * 2,
        out_shape=[jax.ShapeDtypeStruct((CH, 64, 512), f32)] * 2,
        scratch_shapes=[pltpu.VMEM((block, 128, 512), f32)],
        compiler_params=params(),
        cost_estimate=cost(2**32, 80 * 2**20),
        name="incoming",
    )(h, *left, *parts)


def normalize_rows(load, scr):
    for g in range(ROWS // 8):
        zero = jnp.zeros((8, 128), f32)

        def add(q, sums):
            sums = list(sums)
            for u in range(16):
                sums[u % 4] += load(q * 16 + u, g)
            return tuple(sums)

        s = lax.fori_loop(0, CH // 16, add, (zero,) * 4)
        mean = (s[0] + s[1] + s[2] + s[3]) * (1.0 / CH)

        def add_square(q, sums):
            sums = list(sums)
            for u in range(16):
                centred = load(q * 16 + u, g) - mean
                sums[u % 4] += centred * centred
            return tuple(sums)

        s = lax.fori_loop(0, CH // 16, add_square, (zero,) * 4)
        rstd = lax.rsqrt((s[0] + s[1] + s[2] + s[3]) * (1.0 / CH) + LN_EPS)

        def put(q, carry):
            for u in range(16):
                c = q * 16 + u
                scr[pl.ds(8 * g * ROW_PITCH + c, 8, stride=ROW_PITCH), :] = (load(c, g) - mean) * rstd
            return carry

        lax.fori_loop(0, CH // 16, put, 0)


def pair_of(ref, p):
    return jnp.concatenate([ref[2 * p], ref[2 * p + 1]], axis=1)


def update_pair(p, scr, zt_ref, znt_ref, wo_ref, wg_ref, scale, offset, ones):
    start = pl.multiple_of(2 * p * ROW_PITCH, 8)
    normed = jnp.concatenate([scr[pl.ds(start, CH), :], scr[pl.ds(start + ROW_PITCH, CH), :]], axis=1)
    u = (normed * scale + offset).astype(bf16)
    update = jnp.dot(wo_ref[...], extend(u, ones), preferred_element_type=f32)
    gate = jnp.dot(wg_ref[...], extend(pair_of(znt_ref, p), ones), preferred_element_type=f32)
    return (pair_of(zt_ref, p).astype(f32) + (jnp.tanh(gate) + 1.0) * update).astype(bf16)


def finish_project_body(with_left, with_pair, g_ref, o_ref, zt_ref, znt_ref, m_ref, wo_ref, wg_ref, so_ref, oo_ref,
                        w_ref, si_ref, oi_ref, *refs):
    refs = list(refs)
    b_ref = refs.pop(0)
    a_ref = refs.pop(0) if with_left else None
    z1_ref, zn1_ref = (refs.pop(0), refs.pop(0)) if with_pair else (None, None)
    scr, scr2, exts = refs
    normalize_rows(lambda c, g: o_ref[c, 8 * g:8 * g + 8, :], scr)
    scale_out, offset_out = twice(so_ref), twice(oo_ref)
    scale_in, offset_in = twice(si_ref), twice(oi_ref)
    ones = jnp.ones((1, 256), f32)

    def put(p):
        def store(q, t, tile):
            scr2[pl.ds(8 * q * PITCH + 2 * p + t, 8, stride=PITCH), :] = tile
        return store

    def pair(p, carry):
        z1 = update_pair(p, scr, zt_ref, znt_ref, wo_ref, wg_ref, scale_out, offset_out, ones)
        zn1 = norm_columns(z1.astype(f32), scale_in, offset_in).astype(bf16)
        if with_pair:
            for t in range(2):
                z1_ref[2 * p + t] = z1[:, 128 * t:128 * t + 128]
                zn1_ref[2 * p + t] = zn1[:, 128 * t:128 * t + 128]
        m = jnp.concatenate([m_ref[pl.ds(2 * p, 1), :], m_ref[pl.ds(2 * p + 1, 1), :]], axis=1)
        ext = extend(zn1 * m.astype(bf16), m)
        if with_left:
            exts[p] = ext
        store_gated(jnp.dot(w_ref[2 * CH:], ext, preferred_element_type=f32), put(p))
        return carry

    def emit(out):
        def channel(q, carry):
            for u in range(8):
                c = q * 8 + u
                out[c] = scr2[pl.ds(pl.multiple_of(c * PITCH, 8), ROWS), :].astype(bf16)
            return carry

        lax.fori_loop(0, CH // 8, channel, 0)

    lax.fori_loop(0, ROWS // 2, pair, 0, unroll=4)
    emit(b_ref)
    if with_left:
        @pl.when(pl.program_id(1) == 0)
        def _():
            def left(p, carry):
                store_gated(jnp.dot(w_ref[:2 * CH], exts[p], preferred_element_type=f32), put(p))
                return carry

            lax.fori_loop(0, ROWS // 2, left, 0, unroll=4)
            emit(a_ref)


def finish_project(chip, o, at_row, first, zt, znt, m, layer1, layer2, with_pair):
    rows = zt.shape[0]
    n = o.shape[2] // 128
    with_left = first == 0
    natural = lambda j, g: (j + first) ^ g[0]
    out_specs = [pl.BlockSpec((CH, ROWS, 128), lambda i, j, g: (0, i, j))]
    out_shape = [jax.ShapeDtypeStruct((CH, rows, n * 128), bf16)]
    if with_left:
        out_specs.append(pl.BlockSpec((CH, ROWS, 128), lambda i, j, g: (0, i, 0)))
        out_shape.append(jax.ShapeDtypeStruct((CH, rows, 128), bf16))
    if with_pair:
        out_specs += [pl.BlockSpec((ROWS, CH, 128), lambda i, j, g: (i, 0, j))] * 2
        out_shape += [jax.ShapeDtypeStruct((rows, CH, n * 128), bf16)] * 2
    positions = pl.BlockSpec((ROWS, CH, 128), lambda i, j, g: (i, 0, natural(j, g)))
    out = pl.pallas_call(
        functools.partial(finish_project_body, with_left, with_pair),
        grid_spec=pltpu.PrefetchScalarGridSpec(
            num_scalar_prefetch=1,
            grid=(rows // ROWS, n),
            in_specs=[pl.BlockSpec((CH, ROWS, 128), lambda i, j, g: (0, i + at_row // ROWS, j)),
                      positions, positions,
                      pl.BlockSpec((ROWS, 128), lambda i, j, g: (i, natural(j, g))),
                      whole(CH, EXT), whole(CH, EXT), whole(CH, CH), whole(CH, CH),
                      whole(4 * CH, EXT), whole(CH, CH), whole(CH, CH)],
            out_specs=out_specs,
            scratch_shapes=[pltpu.VMEM((ROWS * ROW_PITCH, 128), f32), pltpu.VMEM((CH * PITCH, 128), f32),
                            pltpu.VMEM((ROWS // 2, EXT, 256), bf16)],
        ),
        out_shape=out_shape,
        compiler_params=params(2),
        cost_estimate=cost(rows * n * 128 * 2**19, rows * n * 128 * 1600),
        name="finish_project",
    )(chip, o, zt, znt, m, layer1["w_out"], layer1["w_gate"], layer1["ln_out"][0], layer1["ln_out"][1],
      layer2["w_proj"], layer2["ln_in"][0], layer2["ln_in"][1])
    out = list(out)
    return (out.pop(0), out.pop(0) if with_left else None, out.pop(0) if with_pair else None,
            out.pop(0) if with_pair else None)


def finish_body(g_ref, o_ref, r_ref, zt_ref, znt_ref, wo_ref, wg_ref, so_ref, oo_ref, out_ref, scr, total):
    def add(q, carry):
        for u in range(8):
            total[q * 8 + u] = o_ref[q * 8 + u] + r_ref[q * 8 + u]
        return carry

    lax.fori_loop(0, CH // 8, add, 0)
    normalize_rows(lambda c, g: total[c, 8 * g:8 * g + 8, :], scr)
    scale, offset = twice(so_ref), twice(oo_ref)
    ones = jnp.ones((1, 256), f32)

    def pair(p, carry):
        z2 = update_pair(p, scr, zt_ref, znt_ref, wo_ref, wg_ref, scale, offset, ones).T
        for t in range(2):
            out_ref[2 * p + t] = z2[128 * t:128 * t + 128]
        return carry

    lax.fori_loop(0, ROWS // 2, pair, 0, unroll=4)


def finish(chip, o, received, zt, znt, layer2):
    _, rows, cols = o.shape
    part = pl.BlockSpec((CH, ROWS, 128), lambda i, j, g: (0, i, j))
    positions = pl.BlockSpec((ROWS, CH, 128), lambda i, j, g: (i, 0, j))
    return pl.pallas_call(
        finish_body,
        grid_spec=pltpu.PrefetchScalarGridSpec(
            num_scalar_prefetch=1,
            grid=(rows // ROWS, cols // 128),
            in_specs=[part, part, positions, positions,
                      whole(CH, EXT), whole(CH, EXT), whole(CH, CH), whole(CH, CH)],
            out_specs=pl.BlockSpec((ROWS, 128, CH), lambda i, j, g: (i, j ^ g[0], 0)),
            scratch_shapes=[pltpu.VMEM((ROWS * ROW_PITCH, 128), f32), pltpu.VMEM((CH, ROWS, 128), f32)],
        ),
        out_shape=jax.ShapeDtypeStruct((rows, cols, CH), bf16),
        compiler_params=params(2),
        cost_estimate=cost(rows * cols * 2**17, rows * cols * 1800),
        name="finish",
    )(chip, o, received, zt, znt, layer2["w_out"], layer2["w_gate"], layer2["ln_out"][0], layer2["ln_out"][1])


def with_bias(w, b):
    n = w.shape[1]
    return jnp.concatenate([w.T, b[:, None], jnp.zeros((n, EXT - CH - 1), bf16)], axis=1) * jnp.asarray(0.5, bf16)


def layer_params(ln_in, w_proj, b_proj, w_gate, b_gate, ln_out, w_out, b_out):
    lanes = lambda v: jnp.broadcast_to(v.astype(f32)[:, None], (CH, CH))
    proj = with_bias(w_proj, b_proj).reshape(2, 2, CH // 8, 8, EXT).transpose(0, 2, 1, 3, 4).reshape(4 * CH, EXT)
    gate, out = with_bias(w_gate, b_gate), with_bias(w_out, b_out)
    return {"w_proj": proj, "w_gate": gate, "w_out": out,
            "ln_in": (lanes(ln_in[0]), lanes(ln_in[1])), "ln_out": (lanes(ln_out[0]), lanes(ln_out[1]))}


def solution(mesh):
    row_spec = P(("batch", "dap"), None, None)
    mask_spec = P(("batch", "dap"), None)
    n = mesh.shape["dap"]

    def swap(x, bits):
        return lax.ppermute(x, "dap", [(i, i ^ bits) for i in range(n)])

    def local_layers(pair, pair_mask, ln_in, w_proj, b_proj, w_gate, b_gate, ln_out, w_out, b_out):
        layer1, layer2 = (layer_params(ln_in[l], w_proj[l], b_proj[l], w_gate[l], b_gate[l], ln_out[l], w_out[l],
                                       b_out[l]) for l in range(2))
        me = lax.axis_index("dap")
        chip, core = (me // 2).reshape(1).astype(jnp.int32), (me % 2).reshape(1).astype(jnp.int32)
        half = pair.shape[0] // 2

        mask = pair_mask.astype(f32)
        masks = [mask, swap(mask, 2), swap(mask, 4), swap(mask, 6)]
        pairs = [pair, swap(pair, 2), swap(pair, 4)]
        pairs.append(jnp.concatenate([swap(pairs[1][:half], 4), swap(pairs[2][half:], 2)], axis=0))

        left, mine, theirs, zt, znt = [], [], [], [], []
        b2, a2 = [[], [], [], []], []
        z1 = zn1 = None
        for s in range(4):
            a, b, t, tn = project(pairs[s], masks[s], layer1["w_proj"], *layer1["ln_in"])
            left.append(a)
            mine.append(b)
            theirs.append(swap(b, 1))
            zt.append(t)
            znt.append(tn)
        for rows, cols in RECTS:
            o = outgoing(core, [left[s] for s in rows], [mine[s] for s in cols], [theirs[s] for s in cols])
            for at, s in enumerate(rows):
                b, a, zz, zzn = finish_project(chip, o, 64 * at, cols[0], zt[s], znt[s], masks[s], layer1, layer2, s == 0)
                b2[s].append(b)
                if a is not None:
                    a2.append(a)
                if s == 0:
                    z1, zn1 = zz, zzn
        keep, send = incoming(core, a2, b2)
        return finish(chip, keep, swap(send, 1), z1, zn1, layer2)

    return jax.shard_map(local_layers, mesh=mesh,
                         in_specs=(row_spec, mask_spec, P(), P(), P(), P(), P(), P(), P(), P()),
                         out_specs=row_spec, check_vma=False)


RECTS = (((0, 1, 2, 3), (0, 1, 2, 3)),)
```

```python
import functools

import jax
import jax.numpy as jnp
from jax import lax
from jax.experimental import pallas as pl
from jax.experimental.pallas import tpu as pltpu
from jax.sharding import PartitionSpec as P


f32, bf16 = jnp.float32, jnp.bfloat16
LN_EPS = 1e-5
CH = 128
EXT = CH + 16
ROWS = 16
PITCH = 24
ROW_PITCH = 136
VMEM = 56 * 2**20


def norm_columns(x, scale, offset):
    mean = jnp.sum(x, axis=0, keepdims=True) * (1.0 / CH)
    centred = x - mean
    var = jnp.sum(centred * centred, axis=0, keepdims=True) * (1.0 / CH)
    return centred * lax.rsqrt(var + LN_EPS) * scale + offset


def extend(columns, row):
    n = columns.shape[1]
    first = lax.broadcasted_iota(jnp.int32, (16, n), 0) == 0
    extra = jnp.where(first, jnp.broadcast_to(row, (16, n)), 0.0).astype(bf16)
    return jnp.concatenate([columns, extra], axis=0)


def twice(ref):
    return jnp.concatenate([ref[...]] * 2, axis=1)


def store_gated(proj, store):
    for q in range(proj.shape[0] // 16):
        value, gate = proj[16 * q:16 * q + 8], proj[16 * q + 8:16 * q + 16]
        side = (jnp.tanh(gate) + 1.0) * value
        for t in range(2):
            store(q, t, side[:, 128 * t:128 * t + 128])


def piece_start(chip, slot, piece):
    core, half = piece // 2, piece % 2
    middle = (slot == 1) | (slot == 2)
    other = jnp.where(middle, half + 1, slot)
    offset = jnp.where(middle, slot - 1, half)
    return pl.multiple_of((other ^ chip) * 128 + core * 64 + offset * 32, 32)


def project_body(g_ref, z_ref, m_ref, w_ref, sc_ref, of_ref, *refs):
    a_ref, zt_ref, znt_ref, b_ref, scr = refs[-5:]
    starts = [piece_start(g_ref[0], 2 * pl.program_id(1) + p // 4, p % 4) for p in range(8)]
    scale, offset = twice(sc_ref), twice(of_ref)

    def row(i, carry):
        zt = jnp.concatenate([z_ref[i, pl.ds(start, 32), :] for start in starts], axis=0).T
        zt_ref[i] = zt
        zn = norm_columns(zt.astype(f32), scale, offset).astype(bf16)
        znt_ref[i] = zn
        m = m_ref[pl.ds(i, 1), :]
        proj = jnp.dot(w_ref[...], extend(zn * m.astype(bf16), m), preferred_element_type=f32)

        def store(q, t, tile):
            scr[t, pl.ds(8 * q * PITCH + i, 8, stride=PITCH), :] = tile

        store_gated(proj, store)
        return carry

    lax.fori_loop(0, ROWS, row, 0, unroll=8)
    for side, out in ((0, a_ref), (1, b_ref)):
        def channel(q, carry):
            for u in range(16):
                c = q * 16 + u
                start = pl.multiple_of((side * CH + c) * PITCH, 8)
                for t in range(2):
                    out[c, :, 128 * t:128 * t + 128] = scr[t, pl.ds(start, ROWS), :].astype(bf16)
            return carry

        lax.fori_loop(0, CH // 16, channel, 0)


def whole(*shape):
    return pl.BlockSpec(shape, lambda *ids: (0,) * len(shape))


def params(n=1):
    return pltpu.CompilerParams(dimension_semantics=("arbitrary",) * n, vmem_limit_bytes=VMEM)


def cost(flops, nbytes):
    return pl.CostEstimate(flops=flops, bytes_accessed=nbytes, transcendentals=0)


ANY = pl.BlockSpec(memory_space=pl.ANY)


def project(chip, z, m, w, scale, offset, row, slot_rows, filled):
    rows, cols, _ = z.shape
    all_rows = m.shape[0]
    first, slot_first = row // ROWS, row % slot_rows // ROWS
    side = lambda at: pl.BlockSpec((CH, ROWS, 256), lambda i, k: (0, i + at, k))
    return pl.pallas_call(
        project_body,
        grid=(rows // ROWS, cols // 256),
        in_specs=[pl.BlockSpec(memory_space=pltpu.SMEM),
                  pl.BlockSpec((ROWS, cols, CH), lambda i, k: (i, 0, 0)),
                  pl.BlockSpec((ROWS, 256), lambda i, k: (i + first, k)),
                  whole(4 * CH, EXT), whole(CH, CH), whole(CH, CH)] + [ANY] * len(filled),
        out_specs=[side(first)] + [pl.BlockSpec((ROWS, CH, 256), lambda i, k: (i + first, 0, k))] * 2 + [side(slot_first)],
        out_shape=[jax.ShapeDtypeStruct((CH, all_rows, cols), bf16)]
        + [jax.ShapeDtypeStruct((all_rows, CH, cols), bf16)] * 2 + [jax.ShapeDtypeStruct((CH, slot_rows, cols), bf16)],
        input_output_aliases={6 + k: k for k in range(len(filled))},
        scratch_shapes=[pltpu.VMEM((2, 2 * CH * PITCH, 128), f32)],
        compiler_params=params(2),
        cost_estimate=cost(rows * cols * 2**19, rows * cols * 1200),
        name="project",
    )(chip, z, m, w, scale, offset, *filled)


def incoming_body(h_ref, a_ref, b_ref, keep_ref, send_ref, scr):
    at_mine, at_theirs = pl.multiple_of(64 * h_ref[0], 64), pl.multiple_of(64 - 64 * h_ref[0], 64)
    for c in range(keep_ref.shape[0]):
        scr[c] = lax.dot_general(a_ref[c], b_ref[c], (((0,), (0,)), ((), ())), preferred_element_type=f32)
        keep_ref[c] = scr[c, pl.ds(at_mine, 64), :]
        send_ref[c] = scr[c, pl.ds(at_theirs, 64), :]


def incoming(h, a, b, part, width):
    block = 16
    out = jax.ShapeDtypeStruct((CH, 64, width), f32)
    return pl.pallas_call(
        incoming_body,
        grid=(CH // block,),
        in_specs=[pl.BlockSpec(memory_space=pltpu.SMEM),
                  pl.BlockSpec((block,) + a.shape[1:], lambda c: (c, 0, 0)),
                  pl.BlockSpec((block, b.shape[1], width), lambda c: (c, 0, part))],
        out_specs=[pl.BlockSpec((block, 64, width), lambda c: (c, 0, 0))] * 2,
        out_shape=[out, out],
        scratch_shapes=[pltpu.VMEM((block, 128, width), f32)],
        compiler_params=params(),
        cost_estimate=cost(2**23 * width, 160 * 2**10 * width),
        name="incoming",
    )(h, a, b)


def normalize_rows(load, scr):
    groups = range(ROWS // 8)
    for gs in ([list(groups)] if 1 else [[g] for g in groups]):
        zeros = tuple(jnp.zeros((8, 128), f32) for _ in range(4 * len(gs)))

        def add(q, sums):
            sums = list(sums)
            for u in range(64):
                for n, g in enumerate(gs):
                    sums[4 * n + u % 4] += load(q * 64 + u, g)
            return tuple(sums)

        def total(s, n):
            s = list(s[4 * n:4 * n + 4])
            while len(s) > 1:
                s = [s[2 * k] + s[2 * k + 1] for k in range(len(s) // 2)]
            return s[0] * (1.0 / CH)

        s = lax.fori_loop(0, CH // 64, add, zeros)
        means = [total(s, n) for n in range(len(gs))]

        def add_square(q, sums):
            sums = list(sums)
            for u in range(64):
                for n, g in enumerate(gs):
                    centred = load(q * 64 + u, g) - means[n]
                    sums[4 * n + u % 4] += centred * centred
            return tuple(sums)

        s = lax.fori_loop(0, CH // 64, add_square, zeros)
        rstds = [lax.rsqrt(total(s, n) + LN_EPS) for n in range(len(gs))]

        def put(q, carry):
            for u in range(64):
                c = q * 64 + u
                for n, g in enumerate(gs):
                    scr[pl.ds(8 * g * ROW_PITCH + c, 8, stride=ROW_PITCH), :] = (load(c, g) - means[n]) * rstds[n]
            return carry

        lax.fori_loop(0, CH // 64, put, 0)


def pair_of(ref, p):
    return jnp.concatenate([ref[2 * p], ref[2 * p + 1]], axis=1)


def update_pair(p, scr, zt_ref, znt_ref, wo_ref, wg_ref, scale, offset, ones):
    start = pl.multiple_of(2 * p * ROW_PITCH, 8)
    normed = jnp.concatenate([scr[pl.ds(start, CH), :], scr[pl.ds(start + ROW_PITCH, CH), :]], axis=1)
    u = (normed * scale + offset).astype(bf16)
    update = jnp.dot(wo_ref[...], extend(u, ones), preferred_element_type=f32)
    gate = jnp.dot(wg_ref[...], extend(pair_of(znt_ref, p), ones), preferred_element_type=f32)
    return (pair_of(zt_ref, p).astype(f32) + (jnp.tanh(gate) + 1.0) * update).astype(bf16)


def block_body(n, with_left, with_pair, h_ref, a_ref, *refs):
    mine, theirs, refs = refs[:n], refs[n:2 * n], list(refs[2 * n:])
    sums, both = refs[-2:]
    step = pl.program_id(0)
    per_step = a_ref.shape[0]
    sum_steps = CH // per_step

    @pl.when(step < sum_steps)
    def _():
        at_mine, at_theirs = pl.multiple_of(64 * h_ref[0], 64), pl.multiple_of(64 - 64 * h_ref[0], 64)

        def channel(c, carry):
            for s in range(n):
                both[c, pl.ds(128 * s + at_mine, 64), :] = mine[s][c]
                both[c, pl.ds(128 * s + at_theirs, 64), :] = theirs[s][c]
            o = lax.dot_general(a_ref[c], both[c], (((1,), (1,)), ((), ())), preferred_element_type=f32)
            for s in range(n):
                sums[s, step * per_step + c] = o[:, 128 * s:128 * s + 128]
            return carry

        lax.fori_loop(0, per_step, channel, 0, unroll=4)

    @pl.when(step >= sum_steps)
    def _():
        at = step - sum_steps
        tile, row = at % n, pl.multiple_of(at // n * ROWS, ROWS)
        finish_project_body(with_left, with_pair, tile, lambda c, g: sums[tile, c, pl.ds(row + 8 * g, 8), :], *refs[:-2])


def finish_project_body(with_left, with_pair, tile, load, zt_ref, znt_ref, m_ref, wo_ref, wg_ref, so_ref, oo_ref,
                        w_ref, si_ref, oi_ref, *refs):
    refs = list(refs)[-(4 + with_left + 2 * with_pair):]
    b_ref = refs.pop(0)
    z1_ref, zn1_ref = (refs.pop(0), refs.pop(0)) if with_pair else (None, None)
    a_ref = refs.pop(0) if with_left else None
    scr, scr2, exts = refs
    normalize_rows(load, scr)
    scale_out, offset_out = twice(so_ref), twice(oo_ref)
    scale_in, offset_in = twice(si_ref), twice(oi_ref)
    ones = jnp.ones((1, 256), f32)

    def put(p):
        def store(q, t, tile):
            scr2[pl.ds(8 * q * PITCH + 2 * p + t, 8, stride=PITCH), :] = tile

        return store

    def pair(p, carry):
        z1 = update_pair(p, scr, zt_ref, znt_ref, wo_ref, wg_ref, scale_out, offset_out, ones)
        zn1 = norm_columns(z1.astype(f32), scale_in, offset_in).astype(bf16)
        if with_pair:
            for t in range(2):
                z1_ref[2 * p + t] = z1[:, 128 * t:128 * t + 128]
                zn1_ref[2 * p + t] = zn1[:, 128 * t:128 * t + 128]
        m = jnp.concatenate([m_ref[pl.ds(2 * p, 1), :], m_ref[pl.ds(2 * p + 1, 1), :]], axis=1)
        ext = extend(zn1 * m.astype(bf16), m)
        if with_left:
            exts[p] = ext
        store_gated(jnp.dot(w_ref[2 * CH:], ext, preferred_element_type=f32), put(p))
        return carry

    def emit(out):
        def channel(q, carry):
            for u in range(32):
                c = q * 32 + u
                out[c] = scr2[pl.ds(pl.multiple_of(c * PITCH, 8), ROWS), :].astype(bf16)
            return carry

        lax.fori_loop(0, CH // 32, channel, 0)

    lax.fori_loop(0, ROWS // 2, pair, 0, unroll=8)
    emit(b_ref)
    if with_left:
        @pl.when(tile == 0)
        def _():
            def left(p, carry):
                store_gated(jnp.dot(w_ref[:2 * CH], exts[p], preferred_element_type=f32), put(p))
                return carry

            lax.fori_loop(0, ROWS // 2, left, 0, unroll=8)
            emit(a_ref)


def block(core, a, mine, theirs, zt, znt, m, row, rows, first, ln_out, layer1, layer2, with_pair, filled):
    n, per_step = len(mine), 16
    all_rows, _, cols = zt.shape
    with_left = first == 0
    sum_steps, row_block = CH // per_step, row // ROWS

    def at(index):
        def block_index(t):
            f = jnp.maximum(t - sum_steps, 0)
            return index(row_block + f // n, first + f % n)

        return block_index

    def sides(rows, block):
        return pl.BlockSpec((per_step, rows, cols), lambda t: (jnp.minimum(t, sum_steps - 1), block, 0))

    positions = pl.BlockSpec((ROWS, CH, 128), at(lambda i, j: (i, 0, j)))
    out_specs = [pl.BlockSpec((CH, ROWS, 128), at(lambda i, j: (0, i, j)))]
    out_shape = [jax.ShapeDtypeStruct((CH, all_rows, cols), bf16)]
    if with_pair:
        out_specs += [positions] * 2
        out_shape += [jax.ShapeDtypeStruct((all_rows, CH, cols), bf16)] * 2
    if with_left:
        out_specs.append(pl.BlockSpec((CH, ROWS, 128), at(lambda i, j: (0, i, 0))))
        out_shape.append(jax.ShapeDtypeStruct((CH, all_rows, 128), bf16))
    return pl.pallas_call(
        functools.partial(block_body, n, with_left, with_pair),
        grid=(sum_steps + rows // ROWS * n,),
        in_specs=[pl.BlockSpec(memory_space=pltpu.SMEM), sides(rows, row // rows)] + [sides(64, 0)] * (2 * n)
        + [positions, positions, pl.BlockSpec((ROWS, 128), at(lambda i, j: (i, j))),
           whole(CH, EXT), whole(CH, EXT), whole(CH, CH), whole(CH, CH),
           whole(4 * CH, EXT), whole(CH, CH), whole(CH, CH)] + [ANY] * len(filled),
        out_specs=out_specs,
        out_shape=out_shape,
        scratch_shapes=[pltpu.VMEM((ROWS * ROW_PITCH, 128), f32), pltpu.VMEM((CH * PITCH, 128), f32),
                        pltpu.VMEM((ROWS // 2, EXT, 256), bf16),
                        pltpu.VMEM((n, CH, rows, 128), f32), pltpu.VMEM((per_step, 128 * n, cols), bf16)],
        input_output_aliases={12 + 2 * n + k: k for k in range(len(filled))},
        compiler_params=params(),
        cost_estimate=cost(rows * n * 128 * 2**19, rows * n * 128 * 1600),
        name="block",
    )(core, a, *mine, *theirs, zt, znt, m, layer1["w_out"], layer1["w_gate"], ln_out[0], ln_out[1],
      layer2["w_proj"], layer2["ln_in"][0], layer2["ln_in"][1], *filled)


def finish_body(slot0, g_ref, o_ref, r_ref, zt_ref, znt_ref, wo_ref, wg_ref, so_ref, oo_ref, *refs):
    out_ref, scr, total, rows_out, sems = refs[-5:]
    step, last = pl.program_id(0) * pl.num_programs(1) + pl.program_id(1), pl.num_programs(0) * pl.num_programs(1) - 1
    buffer = step % 2

    def copies(step):
        i, slot, buffer = step // pl.num_programs(1), slot0 + step % pl.num_programs(1), step % 2
        row = pl.multiple_of(i * ROWS, ROWS)
        return [pltpu.make_async_copy(rows_out.at[buffer, :, pl.ds(32 * p, 32), :],
                                      out_ref.at[pl.ds(row, ROWS), pl.ds(piece_start(g_ref[0], slot, p), 32), :],
                                      sems.at[buffer, p]) for p in range(4)]

    def add(q, carry):
        for u in range(8):
            total[q * 8 + u] = o_ref[q * 8 + u] + r_ref[q * 8 + u]
        return carry

    lax.fori_loop(0, CH // 8, add, 0)
    normalize_rows(lambda c, g: total[c, 8 * g:8 * g + 8, :], scr)
    scale, offset = twice(so_ref), twice(oo_ref)
    ones = jnp.ones((1, 256), f32)

    def pair(p, carry):
        z2 = update_pair(p, scr, zt_ref, znt_ref, wo_ref, wg_ref, scale, offset, ones).T
        for t in range(2):
            rows_out[buffer, 2 * p + t] = z2[128 * t:128 * t + 128]
        return carry

    lax.fori_loop(0, ROWS // 2, pair, 0, unroll=8)
    for copy in copies(step):
        copy.start()

    @pl.when(step > 0)
    def _():
        for copy in copies(step - 1):
            copy.wait()

    @pl.when(step == last)
    def _():
        for copy in copies(step):
            copy.wait()


def finish(chip, o, received, zt, znt, layer2, part, filled):
    _, rows, cols = o.shape
    n = cols // 128
    sums = pl.BlockSpec((CH, ROWS, 128), lambda i, j: (0, i, j))
    positions = pl.BlockSpec((ROWS, CH, 128), lambda i, j: (i, 0, j + n * part))
    return pl.pallas_call(
        functools.partial(finish_body, n * part),
        grid=(rows // ROWS, n),
        in_specs=[pl.BlockSpec(memory_space=pltpu.SMEM), sums, sums, positions, positions,
                  whole(CH, EXT), whole(CH, EXT), whole(CH, CH), whole(CH, CH)] + [ANY] * len(filled),
        out_specs=ANY,
        out_shape=jax.ShapeDtypeStruct((rows, zt.shape[2], CH), bf16),
        input_output_aliases={9 + k: k for k in range(len(filled))},
        scratch_shapes=[pltpu.VMEM((ROWS * ROW_PITCH, 128), f32), pltpu.VMEM((CH, ROWS, 128), f32),
                        pltpu.VMEM((2, ROWS, 128, CH), bf16), pltpu.SemaphoreType.DMA((2, 4))],
        compiler_params=params(2),
        cost_estimate=cost(rows * cols * 2**17, rows * cols * 1800),
        name="finish",
    )(chip, o, received, zt, znt, layer2["w_out"], layer2["w_gate"], layer2["ln_out"][0], layer2["ln_out"][1], *filled)


def in_slot_order(masks, chip):
    r = masks.reshape(-1, 2, 2, 2, 2, 32)
    r = jnp.where(chip % 2 == 1, r[:, :, ::-1], r)
    r = jnp.where(chip // 2 == 1, r[:, ::-1], r)
    near = jnp.stack([r[:, 0, 1], r[:, 1, 0]], axis=3)
    slots = [r[:, 0, 0], near[:, :, 0], near[:, :, 1], r[:, 1, 1]]
    return jnp.concatenate([slot.reshape(-1, 128) for slot in slots], axis=1)


def with_bias(w, b):
    n = w.shape[1]
    return jnp.concatenate([w.T, b[:, None], jnp.zeros((n, EXT - CH - 1), bf16)], axis=1) * jnp.asarray(0.5, bf16)


def layer_params(ln_in, w_proj, b_proj, w_gate, b_gate, ln_out, w_out, b_out):
    lanes = lambda v: jnp.broadcast_to(v.astype(f32)[:, None], (CH, CH))
    proj = with_bias(w_proj, b_proj).reshape(2, 2, CH // 8, 8, EXT).transpose(0, 2, 1, 3, 4).reshape(4 * CH, EXT)
    gate, out = with_bias(w_gate, b_gate), with_bias(w_out, b_out)
    return {"w_proj": proj, "w_gate": gate, "w_out": out,
            "ln_in": (lanes(ln_in[0]), lanes(ln_in[1])), "ln_out": (lanes(ln_out[0]), lanes(ln_out[1]))}


def solution(mesh):
    row_spec = P(("batch", "dap"), None, None)
    mask_spec = P(("batch", "dap"), None)
    n = mesh.shape["dap"]

    def swap(x, bits):
        return lax.ppermute(x, "dap", [(i, i ^ bits) for i in range(n)])

    def layers(pair, pair_mask, ln_in, w_proj, b_proj, w_gate, b_gate, ln_out, w_out, b_out):
        layer1, layer2 = (layer_params(ln_in[l], w_proj[l], b_proj[l], w_gate[l], b_gate[l], ln_out[l], w_out[l],
                                       b_out[l]) for l in range(2))
        me = lax.axis_index("dap")
        chip, core = (me // 2).reshape(1).astype(jnp.int32), (me % 2).reshape(1).astype(jnp.int32)
        rows = pair.shape[0]
        half = rows // 2

        mask = pair_mask.astype(f32)
        x_mask, y_mask = swap(mask, 2), swap(mask, 4)
        far_mask = swap(mask, 6)
        masks = in_slot_order(jnp.concatenate([mask, x_mask[:half], y_mask[:half], x_mask[half:], y_mask[half:], far_mask]),
                              chip[0])
        top, bottom = lax.optimization_barrier((pair[:half], pair[half:]))
        x_top, y_top = swap(top, 2), swap(top, 4)
        x_bottom, y_bottom = swap(bottom, 2), swap(bottom, 4)
        x_top_on, y_bottom_on, _, _ = lax.optimization_barrier((x_top, y_bottom, x_bottom, y_top))
        pieces = [[pair], [x_top, y_top], [x_bottom, y_bottom],
                  [swap(x_top_on, 4), swap(y_bottom_on, 2)]]

        step = [(top, bottom)]

        def next_step(small):
            return lax.optimization_barrier((small, step[0]))[0]

        def ran(outputs):
            step[0] = outputs[0]
            return outputs

        mine, theirs = [], []
        left = zt = znt = None
        b2 = a2 = None
        z1 = ()
        for s in range(4):
            made = ()
            for at, piece in enumerate(pieces[s]):
                scale, offset = layer1["ln_in"]
                filled = (left, zt, znt) + made if s or at else ()
                left, zt, znt, b = ran(project(chip, piece, masks, layer1["w_proj"], next_step(scale), offset,
                                               rows * s + half * at, rows, filled))
                made = (b,)
            mine.append(b)
            theirs.append(swap(b, 1))
            if s:
                b2, a2 = ran(block(core, left, mine[:s], theirs[:s], zt, znt, masks, rows * s, rows, 0,
                                   next_step(layer1["ln_out"]), layer1, layer2, False, (b2, a2)))
            out = ran(block(core, left, mine[s:], theirs[s:], zt, znt, masks, 0, rows * (s + 1), s,
                            next_step(layer1["ln_out"]), layer1, layer2, True, (b2, *z1) if s else ()))
            b2, z1 = out[0], out[1:3]
            if not s:
                a2 = out[3]

        parts, out = [], ()
        for part in range(2):
            keep, send = ran(incoming(next_step(core), a2, b2, part, 256))
            parts.append((keep, swap(send, 1)))
        for part, (keep, received) in enumerate(parts):
            out = (finish(chip, keep, received, *z1, layer2, part, out),)
        return out[0]

    return jax.shard_map(layers, mesh=mesh,
                         in_specs=(row_spec, mask_spec, P(), P(), P(), P(), P(), P(), P(), P()),
                         out_specs=row_spec, check_vma=False)
```

```python
import functools

import jax
import jax.numpy as jnp
from jax import lax
from jax.experimental import pallas as pl
from jax.experimental.pallas import tpu as pltpu
from jax.sharding import PartitionSpec as P


f32, bf16 = jnp.float32, jnp.bfloat16
LN_EPS = 1e-5
CH = 128
EXT = CH + 16
ROWS = 16
PITCH = 24
ROW_PITCH = 136
VMEM = 56 * 2**20


def norm_columns(x, scale, offset):
    mean = jnp.sum(x, axis=0, keepdims=True) * (1.0 / CH)
    centred = x - mean
    var = jnp.sum(centred * centred, axis=0, keepdims=True) * (1.0 / CH)
    return centred * lax.rsqrt(var + LN_EPS) * scale + offset


def extend(columns, row):
    n = columns.shape[1]
    first = lax.broadcasted_iota(jnp.int32, (16, n), 0) == 0
    extra = jnp.where(first, jnp.broadcast_to(row, (16, n)), 0.0).astype(bf16)
    return jnp.concatenate([columns, extra], axis=0)


def twice(ref):
    return jnp.concatenate([ref[...]] * 2, axis=1)


def store_gated(proj, store):
    for q in range(proj.shape[0] // 16):
        value, gate = proj[16 * q:16 * q + 8], proj[16 * q + 8:16 * q + 16]
        side = (jnp.tanh(gate) + 1.0) * value
        for t in range(2):
            store(q, t, side[:, 128 * t:128 * t + 128])


def piece_start(chip, slot, piece):
    core, half = piece // 2, piece % 2
    middle = (slot == 1) | (slot == 2)
    other = jnp.where(middle, half + 1, slot)
    offset = jnp.where(middle, slot - 1, half)
    return pl.multiple_of((other ^ chip) * 128 + core * 64 + offset * 32, 32)


def project_body(g_ref, z_ref, m_ref, w_ref, sc_ref, of_ref, *refs):
    a_ref, zt_ref, znt_ref, b_ref, scr = refs[-5:]
    starts = [piece_start(g_ref[0], 2 * pl.program_id(1) + p // 4, p % 4) for p in range(8)]
    scale, offset = twice(sc_ref), twice(of_ref)

    def row(i, carry):
        zt = jnp.concatenate([z_ref[i, pl.ds(start, 32), :] for start in starts], axis=0).T
        for t in range(2):
            zt_ref[t, i] = zt[:, 128 * t:128 * t + 128]
        zn = norm_columns(zt.astype(f32), scale, offset).astype(bf16)
        for t in range(2):
            znt_ref[t, i] = zn[:, 128 * t:128 * t + 128]
        m = m_ref[pl.ds(i, 1), :]
        proj = jnp.dot(w_ref[...], extend(zn * m.astype(bf16), m), preferred_element_type=f32)

        def store(q, t, tile):
            scr[t, pl.ds(8 * q * PITCH + i, 8, stride=PITCH), :] = tile

        store_gated(proj, store)
        return carry

    lax.fori_loop(0, ROWS, row, 0, unroll=16)
    for side, out in ((0, a_ref), (1, b_ref)):
        def channel(q, carry):
            for u in range(16):
                c = q * 16 + u
                start = pl.multiple_of((side * CH + c) * PITCH, 8)
                for t in range(2):
                    out[c, :, 128 * t:128 * t + 128] = scr[t, pl.ds(start, ROWS), :].astype(bf16)
            return carry

        lax.fori_loop(0, CH // 16, channel, 0)


def whole(*shape):
    return pl.BlockSpec(shape, lambda *ids: (0,) * len(shape))


def params(n=1):
    return pltpu.CompilerParams(dimension_semantics=("arbitrary",) * n, vmem_limit_bytes=VMEM)


def cost(flops, nbytes):
    return pl.CostEstimate(flops=flops, bytes_accessed=nbytes, transcendentals=0)


ANY = pl.BlockSpec(memory_space=pl.ANY)


def project(chip, z, m, w, scale, offset, row, slot_rows, filled):
    rows, cols, _ = z.shape
    all_rows = m.shape[0]
    first, slot_first = row // ROWS, row % slot_rows // ROWS
    side = lambda at: pl.BlockSpec((CH, ROWS, 256), lambda i, k: (0, i + at, k))
    return pl.pallas_call(
        project_body,
        grid=(rows // ROWS, cols // 256),
        in_specs=[pl.BlockSpec(memory_space=pltpu.SMEM),
                  pl.BlockSpec((ROWS, cols, CH), lambda i, k: (i, 0, 0)),
                  pl.BlockSpec((ROWS, 256), lambda i, k: (i + first, k)),
                  whole(4 * CH, EXT), whole(CH, CH), whole(CH, CH)] + [ANY] * len(filled),
        out_specs=[side(first)] + [pl.BlockSpec((2, ROWS, CH, 128), lambda i, k: (k, i + first, 0, 0))] * 2 + [side(slot_first)],
        out_shape=[jax.ShapeDtypeStruct((CH, all_rows, cols), bf16)]
        + [jax.ShapeDtypeStruct((cols // 128, all_rows, CH, 128), bf16)] * 2
        + [jax.ShapeDtypeStruct((CH, slot_rows, cols), bf16)],
        input_output_aliases={6 + k: k for k in range(len(filled))},
        scratch_shapes=[pltpu.VMEM((2, 2 * CH * PITCH, 128), f32)],
        compiler_params=params(2),
        cost_estimate=cost(rows * cols * 2**19, rows * cols * 1200),
        name="project",
    )(chip, z, m, w, scale, offset, *filled)


def incoming_body(h_ref, a_ref, b_ref, keep_ref, send_ref, scr):
    at_mine, at_theirs = pl.multiple_of(64 * h_ref[0], 64), pl.multiple_of(64 - 64 * h_ref[0], 64)
    for c in range(keep_ref.shape[1]):
        b = jnp.concatenate([b_ref[t, c] for t in range(b_ref.shape[0])], axis=1)
        scr[c] = lax.dot_general(a_ref[c], b, (((0,), (0,)), ((), ())), preferred_element_type=f32)
        for t in range(b_ref.shape[0]):
            keep_ref[t, c] = scr[c, pl.ds(at_mine, 64), 128 * t:128 * t + 128]
            send_ref[t, c] = scr[c, pl.ds(at_theirs, 64), 128 * t:128 * t + 128]


def incoming(h, a, b, part, n):
    block = 16
    out = jax.ShapeDtypeStruct((n, CH, 64, 128), f32)
    return pl.pallas_call(
        incoming_body,
        grid=(CH // block,),
        in_specs=[pl.BlockSpec(memory_space=pltpu.SMEM),
                  pl.BlockSpec((block,) + a.shape[1:], lambda c: (c, 0, 0)),
                  pl.BlockSpec((n, block, b.shape[2], 128), lambda c: (part, c, 0, 0))],
        out_specs=[pl.BlockSpec((n, block, 64, 128), lambda c: (0, c, 0, 0))] * 2,
        out_shape=[out, out],
        scratch_shapes=[pltpu.VMEM((block, 128, 128 * n), f32)],
        compiler_params=params(),
        cost_estimate=cost(2**30 * n, 20 * 2**20 * n),
        name="incoming",
    )(h, a, b)


def normalize_rows(load, scr):
    groups = range(ROWS // 8)
    for gs in ([list(groups)] if 1 else [[g] for g in groups]):
        zeros = tuple(jnp.zeros((8, 128), f32) for _ in range(4 * len(gs)))

        def add(q, sums):
            sums = list(sums)
            for u in range(64):
                for n, g in enumerate(gs):
                    sums[4 * n + u % 4] += load(q * 64 + u, g)
            return tuple(sums)

        def total(s, n):
            s = list(s[4 * n:4 * n + 4])
            while len(s) > 1:
                s = [s[2 * k] + s[2 * k + 1] for k in range(len(s) // 2)]
            return s[0] * (1.0 / CH)

        s = lax.fori_loop(0, CH // 64, add, zeros)
        means = [total(s, n) for n in range(len(gs))]

        def add_square(q, sums):
            sums = list(sums)
            for u in range(64):
                for n, g in enumerate(gs):
                    centred = load(q * 64 + u, g) - means[n]
                    sums[4 * n + u % 4] += centred * centred
            return tuple(sums)

        s = lax.fori_loop(0, CH // 64, add_square, zeros)
        rstds = [lax.rsqrt(total(s, n) + LN_EPS) for n in range(len(gs))]

        def put(q, carry):
            for u in range(64):
                c = q * 64 + u
                for n, g in enumerate(gs):
                    scr[pl.ds(8 * g * ROW_PITCH + c, 8, stride=ROW_PITCH), :] = (load(c, g) - means[n]) * rstds[n]
            return carry

        lax.fori_loop(0, CH // 64, put, 0)


def pair_of(ref, p):
    return jnp.concatenate([ref[2 * p], ref[2 * p + 1]], axis=1)


def update_pair(p, u, zt_ref, znt_ref, wo_ref, wg_ref, ones):
    update = jnp.dot(wo_ref[...], extend(u, ones), preferred_element_type=f32)
    gate = jnp.dot(wg_ref[...], extend(pair_of(znt_ref, p), ones), preferred_element_type=f32)
    return (pair_of(zt_ref, p).astype(f32) + (jnp.tanh(gate) + 1.0) * update).astype(bf16)


def block_body(n, with_left, with_pair, h_ref, a_ref, *refs):
    mine, theirs, refs = refs[:n], refs[n:2 * n], list(refs[2 * n:])
    sums, both = refs[-2:]
    step = pl.program_id(0)
    per_step = a_ref.shape[0]
    sum_steps = CH // per_step

    @pl.when(step < sum_steps)
    def _():
        at_mine, at_theirs = pl.multiple_of(64 * h_ref[0], 64), pl.multiple_of(64 - 64 * h_ref[0], 64)

        def channel(c, carry):
            for s in range(n):
                both[c, pl.ds(128 * s + at_mine, 64), :] = mine[s][c]
                both[c, pl.ds(128 * s + at_theirs, 64), :] = theirs[s][c]
            o = lax.dot_general(a_ref[c], both[c], (((1,), (1,)), ((), ())), preferred_element_type=f32)
            for s in range(n):
                for r in range(0, o.shape[0], 8):
                    to = pl.ds(r * ROW_PITCH + step * per_step + c, 8, stride=ROW_PITCH)
                    sums[s, to, :] = o[r:r + 8, 128 * s:128 * s + 128]
            return carry

        lax.fori_loop(0, per_step, channel, 0, unroll=8)

    @pl.when(step >= sum_steps)
    def _():
        at = step - sum_steps
        tile, row = at % n, pl.multiple_of(at // n * ROWS, ROWS)

        def load(i):
            return sums[tile, pl.ds(pl.multiple_of((row + i) * ROW_PITCH, 8), CH), :]

        finish_project_body(with_left, with_pair, tile, load, *refs[:-2])


def finish_project_body(with_left, with_pair, tile, load, zt_ref, znt_ref, m_ref, wo_ref, wg_ref, so_ref, oo_ref,
                        w_ref, si_ref, oi_ref, *refs):
    refs = list(refs)[-(3 + with_left + 2 * with_pair):]
    b_ref = refs.pop(0).at[0]
    z1_ref, zn1_ref = (refs.pop(0).at[0], refs.pop(0).at[0]) if with_pair else (None, None)
    zt_ref, znt_ref = zt_ref.at[0], znt_ref.at[0]
    a_ref = refs.pop(0) if with_left else None
    scr2, exts = refs
    scale_out, offset_out = twice(so_ref), twice(oo_ref)
    scale_in, offset_in = twice(si_ref), twice(oi_ref)
    ones = jnp.ones((1, 256), f32)

    def put(p):
        def store(q, t, tile):
            scr2[pl.ds(8 * q * PITCH + 2 * p + t, 8, stride=PITCH), :] = tile

        return store

    def pair(p, carry):
        o = jnp.concatenate([load(2 * p), load(2 * p + 1)], axis=1)
        u = norm_columns(o, scale_out, offset_out).astype(bf16)
        z1 = update_pair(p, u, zt_ref, znt_ref, wo_ref, wg_ref, ones)
        zn1 = norm_columns(z1.astype(f32), scale_in, offset_in).astype(bf16)
        if with_pair:
            for t in range(2):
                z1_ref[2 * p + t] = z1[:, 128 * t:128 * t + 128]
                zn1_ref[2 * p + t] = zn1[:, 128 * t:128 * t + 128]
        m = jnp.concatenate([m_ref[pl.ds(2 * p, 1), :], m_ref[pl.ds(2 * p + 1, 1), :]], axis=1)
        ext = extend(zn1 * m.astype(bf16), m)
        if with_left:
            exts[p] = ext
        store_gated(jnp.dot(w_ref[2 * CH:], ext, preferred_element_type=f32), put(p))
        return carry

    def emit(out):
        def channel(q, carry):
            for u in range(32):
                c = q * 32 + u
                out[c] = scr2[pl.ds(pl.multiple_of(c * PITCH, 8), ROWS), :].astype(bf16)
            return carry

        lax.fori_loop(0, CH // 32, channel, 0)

    lax.fori_loop(0, ROWS // 2, pair, 0, unroll=8)
    emit(b_ref)
    if with_left:
        @pl.when(tile == 0)
        def _():
            def left(p, carry):
                store_gated(jnp.dot(w_ref[:2 * CH], exts[p], preferred_element_type=f32), put(p))
                return carry

            lax.fori_loop(0, ROWS // 2, left, 0, unroll=8)
            emit(a_ref)


def block(core, a, mine, theirs, zt, znt, m, row, rows, first, ln_out, layer1, layer2, with_pair, filled):
    n, per_step = len(mine), 16
    slots, all_rows = zt.shape[:2]
    cols = a.shape[2]
    with_left = first == 0
    sum_steps, row_block = CH // per_step, row // ROWS

    def at(index):
        def block_index(t):
            f = jnp.maximum(t - sum_steps, 0)
            return index(row_block + f // n, first + f % n)

        return block_index

    def sides(rows, block):
        return pl.BlockSpec((per_step, rows, cols), lambda t: (jnp.minimum(t, sum_steps - 1), block, 0))

    positions = pl.BlockSpec((1, ROWS, CH, 128), at(lambda i, j: (j, i, 0, 0)))
    out_specs = [pl.BlockSpec((1, CH, ROWS, 128), at(lambda i, j: (j, 0, i, 0)))]
    out_shape = [jax.ShapeDtypeStruct((slots, CH, all_rows, 128), bf16)]
    if with_pair:
        out_specs += [positions] * 2
        out_shape += [jax.ShapeDtypeStruct(zt.shape, bf16)] * 2
    if with_left:
        out_specs.append(pl.BlockSpec((CH, ROWS, 128), at(lambda i, j: (0, i, 0))))
        out_shape.append(jax.ShapeDtypeStruct((CH, all_rows, 128), bf16))
    return pl.pallas_call(
        functools.partial(block_body, n, with_left, with_pair),
        grid=(sum_steps + rows // ROWS * n,),
        in_specs=[pl.BlockSpec(memory_space=pltpu.SMEM), sides(rows, row // rows)] + [sides(64, 0)] * (2 * n)
        + [positions, positions, pl.BlockSpec((ROWS, 128), at(lambda i, j: (i, j))),
           whole(CH, EXT), whole(CH, EXT), whole(CH, CH), whole(CH, CH),
           whole(4 * CH, EXT), whole(CH, CH), whole(CH, CH)] + [ANY] * len(filled),
        out_specs=out_specs,
        out_shape=out_shape,
        scratch_shapes=[pltpu.VMEM((CH * PITCH, 128), f32), pltpu.VMEM((ROWS // 2, EXT, 256), bf16),
                        pltpu.VMEM((n, rows * ROW_PITCH, 128), f32), pltpu.VMEM((per_step, 128 * n, cols), bf16)],
        input_output_aliases={12 + 2 * n + k: k for k in range(len(filled))},
        compiler_params=params(),
        cost_estimate=cost(rows * n * 128 * 2**19, rows * n * 128 * 1600),
        name="block",
    )(core, a, *mine, *theirs, zt, znt, m, layer1["w_out"], layer1["w_gate"], ln_out[0], ln_out[1],
      layer2["w_proj"], layer2["ln_in"][0], layer2["ln_in"][1], *filled)


def finish_body(slot0, g_ref, o_ref, r_ref, zt_ref, znt_ref, wo_ref, wg_ref, so_ref, oo_ref, *refs):
    out_ref, scr, total, rows_out, sems = refs[-5:]
    zt_ref, znt_ref = zt_ref.at[0], znt_ref.at[0]
    step, last = pl.program_id(0) * pl.num_programs(1) + pl.program_id(1), pl.num_programs(0) * pl.num_programs(1) - 1
    buffer = step % 2

    def copies(step):
        i, slot, buffer = step // pl.num_programs(1), slot0 + step % pl.num_programs(1), step % 2
        row = pl.multiple_of(i * ROWS, ROWS)
        return [pltpu.make_async_copy(rows_out.at[buffer, :, pl.ds(32 * p, 32), :],
                                      out_ref.at[pl.ds(row, ROWS), pl.ds(piece_start(g_ref[0], slot, p), 32), :],
                                      sems.at[buffer, p]) for p in range(4)]

    def add(q, carry):
        for u in range(8):
            total[q * 8 + u] = o_ref[0, q * 8 + u] + r_ref[0, q * 8 + u]
        return carry

    lax.fori_loop(0, CH // 8, add, 0)
    normalize_rows(lambda c, g: total[c, 8 * g:8 * g + 8, :], scr)
    scale, offset = twice(so_ref), twice(oo_ref)
    ones = jnp.ones((1, 256), f32)

    def pair(p, carry):
        start = pl.multiple_of(2 * p * ROW_PITCH, 8)
        normed = jnp.concatenate([scr[pl.ds(start, CH), :], scr[pl.ds(start + ROW_PITCH, CH), :]], axis=1)
        u = (normed * scale + offset).astype(bf16)
        z2 = update_pair(p, u, zt_ref, znt_ref, wo_ref, wg_ref, ones).T
        for t in range(2):
            rows_out[buffer, 2 * p + t] = z2[128 * t:128 * t + 128]
        return carry

    lax.fori_loop(0, ROWS // 2, pair, 0, unroll=8)
    for copy in copies(step):
        copy.start()

    @pl.when(step > 0)
    def _():
        for copy in copies(step - 1):
            copy.wait()

    @pl.when(step == last)
    def _():
        for copy in copies(step):
            copy.wait()


def finish(chip, o, received, zt, znt, layer2, part, filled):
    n, _, rows, _ = o.shape
    cols = 128 * n
    sums = pl.BlockSpec((1, CH, ROWS, 128), lambda i, j: (j, 0, i, 0))
    positions = pl.BlockSpec((1, ROWS, CH, 128), lambda i, j: (j + n * part, i, 0, 0))
    return pl.pallas_call(
        functools.partial(finish_body, n * part),
        grid=(rows // ROWS, n),
        in_specs=[pl.BlockSpec(memory_space=pltpu.SMEM), sums, sums, positions, positions,
                  whole(CH, EXT), whole(CH, EXT), whole(CH, CH), whole(CH, CH)] + [ANY] * len(filled),
        out_specs=ANY,
        out_shape=jax.ShapeDtypeStruct((rows, 128 * zt.shape[0], CH), bf16),
        input_output_aliases={9 + k: k for k in range(len(filled))},
        scratch_shapes=[pltpu.VMEM((ROWS * ROW_PITCH, 128), f32), pltpu.VMEM((CH, ROWS, 128), f32),
                        pltpu.VMEM((2, ROWS, 128, CH), bf16), pltpu.SemaphoreType.DMA((2, 4))],
        compiler_params=params(2),
        cost_estimate=cost(rows * cols * 2**17, rows * cols * 1800),
        name="finish",
    )(chip, o, received, zt, znt, layer2["w_out"], layer2["w_gate"], layer2["ln_out"][0], layer2["ln_out"][1], *filled)


def in_slot_order(masks, chip):
    r = masks.reshape(-1, 2, 2, 2, 2, 32)
    r = jnp.where(chip % 2 == 1, r[:, :, ::-1], r)
    r = jnp.where(chip // 2 == 1, r[:, ::-1], r)
    near = jnp.stack([r[:, 0, 1], r[:, 1, 0]], axis=3)
    slots = [r[:, 0, 0], near[:, :, 0], near[:, :, 1], r[:, 1, 1]]
    return jnp.concatenate([slot.reshape(-1, 128) for slot in slots], axis=1)


def with_bias(w, b):
    n = w.shape[1]
    return jnp.concatenate([w.T, b[:, None], jnp.zeros((n, EXT - CH - 1), bf16)], axis=1) * jnp.asarray(0.5, bf16)


def layer_params(ln_in, w_proj, b_proj, w_gate, b_gate, ln_out, w_out, b_out):
    lanes = lambda v: jnp.broadcast_to(v.astype(f32)[:, None], (CH, CH))
    proj = with_bias(w_proj, b_proj).reshape(2, 2, CH // 8, 8, EXT).transpose(0, 2, 1, 3, 4).reshape(4 * CH, EXT)
    gate, out = with_bias(w_gate, b_gate), with_bias(w_out, b_out)
    return {"w_proj": proj, "w_gate": gate, "w_out": out,
            "ln_in": (lanes(ln_in[0]), lanes(ln_in[1])), "ln_out": (lanes(ln_out[0]), lanes(ln_out[1]))}


def solution(mesh):
    row_spec = P(("batch", "dap"), None, None)
    mask_spec = P(("batch", "dap"), None)
    n = mesh.shape["dap"]

    def swap(x, bits):
        return lax.ppermute(x, "dap", [(i, i ^ bits) for i in range(n)])

    def layers(pair, pair_mask, ln_in, w_proj, b_proj, w_gate, b_gate, ln_out, w_out, b_out):
        layer1, layer2 = (layer_params(ln_in[l], w_proj[l], b_proj[l], w_gate[l], b_gate[l], ln_out[l], w_out[l],
                                       b_out[l]) for l in range(2))
        me = lax.axis_index("dap")
        chip, core = (me // 2).reshape(1).astype(jnp.int32), (me % 2).reshape(1).astype(jnp.int32)
        rows = pair.shape[0]
        half = rows // 2

        mask = pair_mask.astype(bf16)
        x_mask, y_mask = swap(mask, 2), swap(mask, 4)
        far_mask = swap(mask, 6)
        masks = in_slot_order(jnp.concatenate([mask, x_mask[:half], y_mask[:half], x_mask[half:], y_mask[half:], far_mask])
                              .astype(f32), chip[0])
        top = pair[:half]
        bottom, _ = lax.optimization_barrier((pair[half:], top))
        x_top, y_top = swap(top, 2), swap(top, 4)
        x_bottom, y_bottom = swap(bottom, 2), swap(bottom, 4)
        x_top_on, y_bottom_on, _, _ = lax.optimization_barrier((x_top, y_bottom, x_bottom, y_top))
        pieces = [[pair], [x_top, y_top], [x_bottom, y_bottom],
                  [swap(x_top_on, 4), swap(y_bottom_on, 2)]]

        step = [(top, bottom)]

        def next_step(small):
            return lax.optimization_barrier((small, step[0]))[0]

        def ran(outputs):
            step[0] = outputs[0]
            return outputs

        mine, theirs = [], []
        left = zt = znt = None
        b2 = a2 = None
        z1 = ()
        for s in range(4):
            made = ()
            for at, piece in enumerate(pieces[s]):
                scale, offset = layer1["ln_in"]
                filled = (left, zt, znt) + made if s or at else ()
                left, zt, znt, b = ran(project(chip, piece, masks, layer1["w_proj"], next_step(scale), offset,
                                               rows * s + half * at, rows, filled))
                made = (b,)
            mine.append(b)
            theirs.append(swap(b, 1))
            if s:
                b2, a2 = ran(block(core, left, mine[:s], theirs[:s], zt, znt, masks, rows * s, rows, 0,
                                   next_step(layer1["ln_out"]), layer1, layer2, False, (b2, a2)))
            out = ran(block(core, left, mine[s:], theirs[s:], zt, znt, masks, 0, rows * (s + 1), s,
                            next_step(layer1["ln_out"]), layer1, layer2, True, (b2, *z1) if s else ()))
            b2, z1 = out[0], out[1:3]
            if not s:
                a2 = out[3]

        parts, out = [], ()
        for part in range(2):
            keep, send = ran(incoming(next_step(core), a2, b2, part, 2))
            parts.append((keep, swap(send, 1)))
        for part, (keep, received) in enumerate(parts):
            out = (finish(chip, keep, received, *z1, layer2, part, out),)
        return out[0]

    return jax.shard_map(layers, mesh=mesh,
                         in_specs=(row_spec, mask_spec, P(), P(), P(), P(), P(), P(), P(), P()),
                         out_specs=row_spec, check_vma=False)
```

```python
import functools

import jax
import jax.numpy as jnp
from jax import lax
from jax.experimental import pallas as pl
from jax.experimental.pallas import tpu as pltpu
from jax.sharding import PartitionSpec as P


f32, bf16 = jnp.float32, jnp.bfloat16
LN_EPS = 1e-5
CH = 128
EXT = CH + 16
ROWS = 16
PITCH = 24
ROW_PITCH = 136
VMEM = 56 * 2**20


def norm_columns(x, scale, offset):
    mean = jnp.sum(x, axis=0, keepdims=True) * (1.0 / CH)
    centred = x - mean
    var = jnp.sum(centred * centred, axis=0, keepdims=True) * (1.0 / CH)
    return centred * lax.rsqrt(var + LN_EPS) * scale + offset


def extend(columns, row):
    n = columns.shape[1]
    first = lax.broadcasted_iota(jnp.int32, (16, n), 0) == 0
    extra = jnp.where(first, jnp.broadcast_to(row, (16, n)), 0.0).astype(bf16)
    return jnp.concatenate([columns, extra], axis=0)


def twice(ref):
    return jnp.concatenate([ref[...]] * 2, axis=1)


def store_gated(proj, store):
    for q in range(proj.shape[0] // 16):
        value, gate = proj[16 * q:16 * q + 8], proj[16 * q + 8:16 * q + 16]
        side = (jnp.tanh(gate) + 1.0) * value
        for t in range(2):
            store(q, t, side[:, 128 * t:128 * t + 128])


def piece_start(chip, slot, piece):
    core, half = piece // 2, piece % 2
    middle = (slot == 1) | (slot == 2)
    other = jnp.where(middle, half + 1, slot)
    offset = jnp.where(middle, slot - 1, half)
    return pl.multiple_of((other ^ chip) * 128 + core * 64 + offset * 32, 32)


def project_body(g_ref, z_ref, m_ref, w_ref, sc_ref, of_ref, *refs):
    a_ref, zt_ref, znt_ref, b_ref, scr = refs[-5:]
    starts = [piece_start(g_ref[0], 2 * pl.program_id(1) + p // 4, p % 4) for p in range(8)]
    scale, offset = twice(sc_ref), twice(of_ref)

    def row(i, carry):
        zt = jnp.concatenate([z_ref[i, pl.ds(start, 32), :] for start in starts], axis=0).T
        for t in range(2):
            zt_ref[t, i] = zt[:, 128 * t:128 * t + 128]
        zn = norm_columns(zt.astype(f32), scale, offset).astype(bf16)
        for t in range(2):
            znt_ref[t, i] = zn[:, 128 * t:128 * t + 128]
        m = m_ref[pl.ds(i, 1), :]
        proj = jnp.dot(w_ref[...], extend(zn * m.astype(bf16), m), preferred_element_type=f32)

        def store(q, t, tile):
            scr[t, pl.ds(8 * q * PITCH + i, 8, stride=PITCH), :] = tile

        store_gated(proj, store)
        return carry

    lax.fori_loop(0, ROWS, row, 0, unroll=16)
    for side, out in ((0, a_ref), (1, b_ref)):
        def channel(q, carry):
            for u in range(16):
                c = q * 16 + u
                start = pl.multiple_of((side * CH + c) * PITCH, 8)
                for t in range(2):
                    out[c, :, 128 * t:128 * t + 128] = scr[t, pl.ds(start, ROWS), :].astype(bf16)
            return carry

        lax.fori_loop(0, CH // 16, channel, 0)


def whole(*shape):
    return pl.BlockSpec(shape, lambda *ids: (0,) * len(shape))


def params(n=1):
    return pltpu.CompilerParams(dimension_semantics=("arbitrary",) * n, vmem_limit_bytes=VMEM)


def cost(flops, nbytes):
    return pl.CostEstimate(flops=flops, bytes_accessed=nbytes, transcendentals=0)


ANY = pl.BlockSpec(memory_space=pl.ANY)


def project(chip, z, m, w, scale, offset, row, slot_rows, all_rows, filled):
    rows, cols, _ = z.shape
    first, slot_first = row // ROWS, row % slot_rows // ROWS
    side = lambda at: pl.BlockSpec((CH, ROWS, 256), lambda i, k: (0, i + at, k))
    return pl.pallas_call(
        project_body,
        grid=(rows // ROWS, cols // 256),
        in_specs=[pl.BlockSpec(memory_space=pltpu.SMEM),
                  pl.BlockSpec((ROWS, cols, CH), lambda i, k: (i, 0, 0)),
                  pl.BlockSpec((ROWS, 256), lambda i, k: (i + first, k)),
                  whole(4 * CH, EXT), whole(CH, CH), whole(CH, CH)] + [ANY] * len(filled),
        out_specs=[side(first)] + [pl.BlockSpec((2, ROWS, CH, 128), lambda i, k: (k, i + first, 0, 0))] * 2 + [side(slot_first)],
        out_shape=[jax.ShapeDtypeStruct((CH, all_rows, cols), bf16)]
        + [jax.ShapeDtypeStruct((cols // 128, all_rows, CH, 128), bf16)] * 2
        + [jax.ShapeDtypeStruct((CH, slot_rows, cols), bf16)],
        input_output_aliases={6 + k: k for k in range(len(filled))},
        scratch_shapes=[pltpu.VMEM((2, 2 * CH * PITCH, 128), f32)],
        compiler_params=params(2),
        cost_estimate=cost(rows * cols * 2**19, rows * cols * 1200),
        name="project",
    )(chip, z, m, w, scale, offset, *filled)


def incoming_body(h_ref, a_ref, b_ref, keep_ref, send_ref, scr):
    at_mine, at_theirs = pl.multiple_of(64 * h_ref[0], 64), pl.multiple_of(64 - 64 * h_ref[0], 64)
    for c in range(keep_ref.shape[1]):
        b = jnp.concatenate([b_ref[t, c] for t in range(b_ref.shape[0])], axis=1)
        scr[c] = lax.dot_general(a_ref[c], b, (((0,), (0,)), ((), ())), preferred_element_type=f32)
        for t in range(b_ref.shape[0]):
            keep_ref[t, c] = scr[c, pl.ds(at_mine, 64), 128 * t:128 * t + 128]
            send_ref[t, c] = scr[c, pl.ds(at_theirs, 64), 128 * t:128 * t + 128]


def incoming(h, a, b, part, n):
    block = 16
    out = jax.ShapeDtypeStruct((n, CH, 64, 128), f32)
    return pl.pallas_call(
        incoming_body,
        grid=(CH // block,),
        in_specs=[pl.BlockSpec(memory_space=pltpu.SMEM),
                  pl.BlockSpec((block,) + a.shape[1:], lambda c: (c, 0, 0)),
                  pl.BlockSpec((n, block, b.shape[2], 128), lambda c: (part, c, 0, 0))],
        out_specs=[pl.BlockSpec((n, block, 64, 128), lambda c: (0, c, 0, 0))] * 2,
        out_shape=[out, out],
        scratch_shapes=[pltpu.VMEM((block, 128, 128 * n), f32)],
        compiler_params=params(),
        cost_estimate=cost(2**30 * n, 20 * 2**20 * n),
        name="incoming",
    )(h, a, b)


def normalize_rows(first_load, load, scr):
    groups = range(ROWS // 8)
    for gs in ([list(groups)] if 1 else [[g] for g in groups]):
        zeros = tuple(jnp.zeros((8, 128), f32) for _ in range(4 * len(gs)))

        def add(q, sums):
            sums = list(sums)
            for u in range(64):
                for n, g in enumerate(gs):
                    sums[4 * n + u % 4] += first_load(q * 64 + u, g)
            return tuple(sums)

        def total(s, n):
            s = list(s[4 * n:4 * n + 4])
            while len(s) > 1:
                s = [s[2 * k] + s[2 * k + 1] for k in range(len(s) // 2)]
            return s[0] * (1.0 / CH)

        s = lax.fori_loop(0, CH // 64, add, zeros)
        means = [total(s, n) for n in range(len(gs))]

        def add_square(q, sums):
            sums = list(sums)
            for u in range(64):
                for n, g in enumerate(gs):
                    centred = load(q * 64 + u, g) - means[n]
                    sums[4 * n + u % 4] += centred * centred
            return tuple(sums)

        s = lax.fori_loop(0, CH // 64, add_square, zeros)
        rstds = [lax.rsqrt(total(s, n) + LN_EPS) for n in range(len(gs))]

        def put(q, carry):
            for u in range(64):
                c = q * 64 + u
                for n, g in enumerate(gs):
                    scr[pl.ds(8 * g * ROW_PITCH + c, 8, stride=ROW_PITCH), :] = (load(c, g) - means[n]) * rstds[n]
            return carry

        lax.fori_loop(0, CH // 64, put, 0)


def pair_of(ref, p):
    return jnp.concatenate([ref[2 * p], ref[2 * p + 1]], axis=1)


def update_pair(p, u, zt_ref, znt_ref, wo_ref, wg_ref, ones):
    update = jnp.dot(wo_ref[...], extend(u, ones), preferred_element_type=f32)
    gate = jnp.dot(wg_ref[...], extend(pair_of(znt_ref, p), ones), preferred_element_type=f32)
    return (pair_of(zt_ref, p).astype(f32) + (jnp.tanh(gate) + 1.0) * update).astype(bf16)


def block_body(n, with_left, with_pair, h_ref, a_ref, *refs):
    mine, theirs, refs = refs[:n], refs[n:2 * n], list(refs[2 * n:])
    sums, both = refs[-2:]
    step = pl.program_id(0)
    per_step = a_ref.shape[0]
    sum_steps = CH // per_step

    @pl.when(step < sum_steps)
    def _():
        at_mine, at_theirs = pl.multiple_of(64 * h_ref[0], 64), pl.multiple_of(64 - 64 * h_ref[0], 64)

        def channel(c, carry):
            for s in range(n):
                both[c, pl.ds(128 * s + at_mine, 64), :] = mine[s][c]
                both[c, pl.ds(128 * s + at_theirs, 64), :] = theirs[s][c]
            o = lax.dot_general(a_ref[c], both[c], (((1,), (1,)), ((), ())), preferred_element_type=f32)
            for s in range(n):
                for r in range(0, o.shape[0], 8):
                    to = pl.ds(r * ROW_PITCH + step * per_step + c, 8, stride=ROW_PITCH)
                    sums[s, to, :] = o[r:r + 8, 128 * s:128 * s + 128]
            return carry

        lax.fori_loop(0, per_step, channel, 0, unroll=8)

    @pl.when(step >= sum_steps)
    def _():
        at = step - sum_steps
        tile, row = at % n, pl.multiple_of(at // n * ROWS, ROWS)

        def load(i):
            return sums[tile, pl.ds(pl.multiple_of((row + i) * ROW_PITCH, 8), CH), :]

        finish_project_body(with_left, with_pair, tile, load, *refs[:-2])


def finish_project_body(with_left, with_pair, tile, load, zt_ref, znt_ref, m_ref, wo_ref, wg_ref, so_ref, oo_ref,
                        w_ref, si_ref, oi_ref, *refs):
    refs = list(refs)[-(4 + with_left + 2 * with_pair):]
    b_ref = refs.pop(0).at[0]
    z1_ref, zn1_ref = (refs.pop(0).at[0], refs.pop(0).at[0]) if with_pair else (None, None)
    zt_ref, znt_ref = zt_ref.at[0], znt_ref.at[0]
    a_ref = refs.pop(0) if with_left else None
    scr2, exts, z1s = refs
    scale_out, offset_out = twice(so_ref), twice(oo_ref)
    scale_in, offset_in = twice(si_ref), twice(oi_ref)
    ones = jnp.ones((1, 256), f32)

    def put(p):
        def store(q, t, tile):
            scr2[pl.ds(8 * q * PITCH + 2 * p + t, 8, stride=PITCH), :] = tile

        return store

    def pair(p, carry):
        o = jnp.concatenate([load(2 * p), load(2 * p + 1)], axis=1)
        u = norm_columns(o, scale_out, offset_out).astype(bf16)
        z1s[p] = update_pair(p, u, zt_ref, znt_ref, wo_ref, wg_ref, ones)
        return carry

    def project_pair(p, carry):
        z1 = z1s[p]
        zn1 = norm_columns(z1.astype(f32), scale_in, offset_in).astype(bf16)
        if with_pair:
            for t in range(2):
                z1_ref[2 * p + t] = z1[:, 128 * t:128 * t + 128]
                zn1_ref[2 * p + t] = zn1[:, 128 * t:128 * t + 128]
        m = jnp.concatenate([m_ref[pl.ds(2 * p, 1), :], m_ref[pl.ds(2 * p + 1, 1), :]], axis=1)
        ext = extend(zn1 * m.astype(bf16), m)
        if with_left:
            exts[p] = ext
        store_gated(jnp.dot(w_ref[2 * CH:], ext, preferred_element_type=f32), put(p))
        return carry

    def emit(out):
        def channel(q, carry):
            for u in range(16):
                c = q * 16 + u
                out[c] = scr2[pl.ds(pl.multiple_of(c * PITCH, 8), ROWS), :].astype(bf16)
            return carry

        lax.fori_loop(0, CH // 16, channel, 0)

    lax.fori_loop(0, ROWS // 2, pair, 0, unroll=8)
    lax.fori_loop(0, ROWS // 2, project_pair, 0, unroll=8)
    emit(b_ref)
    if with_left:
        @pl.when(tile == 0)
        def _():
            def left(p, carry):
                store_gated(jnp.dot(w_ref[:2 * CH], exts[p], preferred_element_type=f32), put(p))
                return carry

            lax.fori_loop(0, ROWS // 2, left, 0, unroll=8)
            emit(a_ref)


def block(core, a, mine, theirs, zt, znt, m, row, rows, first, ln_out, layer1, layer2, with_pair, filled):
    n, per_step = len(mine), 16
    slots, all_rows = zt.shape[:2]
    cols = a.shape[2]
    with_left = first == 0
    sum_steps, row_block = CH // per_step, row // ROWS

    def at(index):
        def block_index(t):
            f = jnp.maximum(t - sum_steps, 0)
            return index(row_block + f // n, first + f % n)

        return block_index

    def sides(rows, block):
        return pl.BlockSpec((per_step, rows, cols), lambda t: (jnp.minimum(t, sum_steps - 1), block, 0))

    positions = pl.BlockSpec((1, ROWS, CH, 128), at(lambda i, j: (j, i, 0, 0)))
    out_specs = [pl.BlockSpec((1, CH, ROWS, 128), at(lambda i, j: (j, 0, i, 0)))]
    out_shape = [jax.ShapeDtypeStruct((slots, CH, all_rows, 128), bf16)]
    if with_pair:
        out_specs += [pl.BlockSpec((1, ROWS, CH, 128), at(lambda i, j: (j, jnp.minimum(i, 64 // ROWS), 0, 0)))] * 2
        out_shape += [jax.ShapeDtypeStruct((slots, 64 + ROWS, CH, 128), bf16)] * 2
    if with_left:
        out_specs.append(pl.BlockSpec((CH, ROWS, 128), at(lambda i, j: (0, i, 0))))
        out_shape.append(jax.ShapeDtypeStruct((CH, all_rows, 128), bf16))
    return pl.pallas_call(
        functools.partial(block_body, n, with_left, with_pair),
        grid=(sum_steps + rows // ROWS * n,),
        in_specs=[pl.BlockSpec(memory_space=pltpu.SMEM), sides(rows, row // rows)] + [sides(64, 0)] * (2 * n)
        + [positions, positions, pl.BlockSpec((ROWS, 128), at(lambda i, j: (i, j))),
           whole(CH, EXT), whole(CH, EXT), whole(CH, CH), whole(CH, CH),
           whole(4 * CH, EXT), whole(CH, CH), whole(CH, CH)] + [ANY] * len(filled),
        out_specs=out_specs,
        out_shape=out_shape,
        scratch_shapes=[pltpu.VMEM((CH * PITCH, 128), f32), pltpu.VMEM((ROWS // 2, EXT, 256), bf16),
                        pltpu.VMEM((ROWS // 2, CH, 256), bf16),
                        pltpu.VMEM((n, rows * ROW_PITCH, 128), f32), pltpu.VMEM((per_step, 128 * n, cols), bf16)],
        input_output_aliases={12 + 2 * n + k: k for k in range(len(filled))},
        compiler_params=params(),
        cost_estimate=cost(rows * n * 128 * 2**19, rows * n * 128 * 1600),
        name="block",
    )(core, a, *mine, *theirs, zt, znt, m, layer1["w_out"], layer1["w_gate"], ln_out[0], ln_out[1],
      layer2["w_proj"], layer2["ln_in"][0], layer2["ln_in"][1], *filled)


def finish_body(slot0, g_ref, o_ref, r_ref, zt_ref, znt_ref, wo_ref, wg_ref, so_ref, oo_ref, *refs):
    out_ref, scr, total, rows_out, sems = refs[-5:]
    zt_ref, znt_ref = zt_ref.at[0], znt_ref.at[0]
    step, last = pl.program_id(0) * pl.num_programs(1) + pl.program_id(1), pl.num_programs(0) * pl.num_programs(1) - 1
    buffer = step % 2

    def copies(step):
        i, slot, buffer = step // pl.num_programs(1), slot0 + step % pl.num_programs(1), step % 2
        row = pl.multiple_of(i * ROWS, ROWS)
        return [pltpu.make_async_copy(rows_out.at[buffer, :, pl.ds(32 * p, 32), :],
                                      out_ref.at[pl.ds(row, ROWS), pl.ds(piece_start(g_ref[0], slot, p), 32), :],
                                      sems.at[buffer, p]) for p in range(4)]

    def add(c, g):
        both = o_ref[0, c, 8 * g:8 * g + 8, :] + r_ref[0, c, 8 * g:8 * g + 8, :]
        total[c, 8 * g:8 * g + 8, :] = both
        return both

    normalize_rows(add, lambda c, g: total[c, 8 * g:8 * g + 8, :], scr)
    scale, offset = twice(so_ref), twice(oo_ref)
    ones = jnp.ones((1, 256), f32)

    def pair(p, carry):
        start = pl.multiple_of(2 * p * ROW_PITCH, 8)
        normed = jnp.concatenate([scr[pl.ds(start, CH), :], scr[pl.ds(start + ROW_PITCH, CH), :]], axis=1)
        u = (normed * scale + offset).astype(bf16)
        z2 = update_pair(p, u, zt_ref, znt_ref, wo_ref, wg_ref, ones).T
        for t in range(2):
            rows_out[buffer, 2 * p + t] = z2[128 * t:128 * t + 128]
        return carry

    lax.fori_loop(0, ROWS // 2, pair, 0, unroll=8)
    for copy in copies(step):
        copy.start()

    @pl.when(step > 0)
    def _():
        for copy in copies(step - 1):
            copy.wait()

    @pl.when(step == last)
    def _():
        for copy in copies(step):
            copy.wait()


def finish(chip, o, received, zt, znt, layer2, part, filled):
    n, _, rows, _ = o.shape
    cols = 128 * n
    sums = pl.BlockSpec((1, CH, ROWS, 128), lambda i, j: (j, 0, i, 0))
    positions = pl.BlockSpec((1, ROWS, CH, 128), lambda i, j: (j + n * part, i, 0, 0))
    return pl.pallas_call(
        functools.partial(finish_body, n * part),
        grid=(rows // ROWS, n),
        in_specs=[pl.BlockSpec(memory_space=pltpu.SMEM), sums, sums, positions, positions,
                  whole(CH, EXT), whole(CH, EXT), whole(CH, CH), whole(CH, CH)] + [ANY] * len(filled),
        out_specs=ANY,
        out_shape=jax.ShapeDtypeStruct((rows, 128 * zt.shape[0], CH), bf16),
        input_output_aliases={9 + k: k for k in range(len(filled))},
        scratch_shapes=[pltpu.VMEM((ROWS * ROW_PITCH, 128), f32), pltpu.VMEM((CH, ROWS, 128), f32),
                        pltpu.VMEM((2, ROWS, 128, CH), bf16), pltpu.SemaphoreType.DMA((2, 4))],
        compiler_params=params(2),
        cost_estimate=cost(rows * cols * 2**17, rows * cols * 1800),
        name="finish",
    )(chip, o, received, zt, znt, layer2["w_out"], layer2["w_gate"], layer2["ln_out"][0], layer2["ln_out"][1], *filled)


def in_slot_order(masks, chip):
    r = masks.reshape(-1, 2, 2, 2, 2, 32)
    r = jnp.where(chip % 2 == 1, r[:, :, ::-1], r)
    r = jnp.where(chip // 2 == 1, r[:, ::-1], r)
    near = jnp.stack([r[:, 0, 1], r[:, 1, 0]], axis=3)
    slots = [r[:, 0, 0], near[:, :, 0], near[:, :, 1], r[:, 1, 1]]
    return jnp.concatenate([slot.reshape(-1, 128) for slot in slots], axis=1)


def with_bias(w, b):
    n = w.shape[1]
    return jnp.concatenate([w.T, b[:, None], jnp.zeros((n, EXT - CH - 1), bf16)], axis=1) * jnp.asarray(0.5, bf16)


def layer_params(ln_in, w_proj, b_proj, w_gate, b_gate, ln_out, w_out, b_out):
    lanes = lambda v: jnp.broadcast_to(v.astype(f32)[:, None], (CH, CH))
    proj = with_bias(w_proj, b_proj).reshape(2, 2, CH // 8, 8, EXT).transpose(0, 2, 1, 3, 4).reshape(4 * CH, EXT)
    gate, out = with_bias(w_gate, b_gate), with_bias(w_out, b_out)
    return {"w_proj": proj, "w_gate": gate, "w_out": out,
            "ln_in": (lanes(ln_in[0]), lanes(ln_in[1])), "ln_out": (lanes(ln_out[0]), lanes(ln_out[1]))}


def solution(mesh):
    row_spec = P(("batch", "dap"), None, None)
    mask_spec = P(("batch", "dap"), None)
    n = mesh.shape["dap"]

    def swap(x, bits):
        return lax.ppermute(x, "dap", [(i, i ^ bits) for i in range(n)])

    def layers(pair, pair_mask, ln_in, w_proj, b_proj, w_gate, b_gate, ln_out, w_out, b_out):
        layer1, layer2 = (layer_params(ln_in[l], w_proj[l], b_proj[l], w_gate[l], b_gate[l], ln_out[l], w_out[l],
                                       b_out[l]) for l in range(2))
        me = lax.axis_index("dap")
        chip, core = (me // 2).reshape(1).astype(jnp.int32), (me % 2).reshape(1).astype(jnp.int32)
        rows = pair.shape[0]
        half = rows // 2

        mask = pair_mask.astype(bf16)
        x_mask, y_mask = swap(mask, 2), swap(mask, 4)
        far_mask = swap(mask, 6)
        own_masks = in_slot_order(mask.astype(f32), chip[0])
        masks = in_slot_order(jnp.concatenate([mask, x_mask[:half], y_mask[:half], x_mask[half:], y_mask[half:], far_mask])
                              .astype(f32), chip[0])
        top = pair[:half]
        bottom = lax.optimization_barrier((pair, top))[0][half:]
        x_top, y_top = swap(top, 2), swap(top, 4)
        x_bottom, y_bottom = swap(bottom, 2), swap(bottom, 4)
        x_top_on, y_bottom_on, _, _ = lax.optimization_barrier((x_top, y_bottom, x_bottom, y_top))
        pieces = [[pair], [x_top, y_top], [x_bottom, y_bottom],
                  [swap(x_top_on, 4), swap(y_bottom_on, 2)]]

        step = [(top, bottom)]

        def next_step(small):
            return lax.optimization_barrier((small, step[0]))[0]

        def ran(outputs):
            step[0] = outputs[0]
            return outputs

        mine, theirs = [], []
        left = zt = znt = None
        b2 = a2 = None
        z1 = ()
        for s in range(4):
            made = ()
            for at, piece in enumerate(pieces[s]):
                scale, offset = layer1["ln_in"]
                filled = (left, zt, znt) + made if s or at else ()
                left, zt, znt, b = ran(project(chip, piece, masks if s else own_masks, layer1["w_proj"], next_step(scale), offset,
                                               rows * s + half * at, rows, 4 * rows, filled))
                made = (b,)
            mine.append(b)
            theirs.append(swap(b, 1))
            if s:
                b2, a2 = ran(block(core, left, mine[:s], theirs[:s], zt, znt, masks, rows * s, rows, 0,
                                   next_step(layer1["ln_out"]), layer1, layer2, False, (b2, a2)))
            out = ran(block(core, left, mine[s:], theirs[s:], zt, znt, masks if s else own_masks, 0, rows * (s + 1), s,
                            next_step(layer1["ln_out"]), layer1, layer2, True, (b2, *z1) if s else ()))
            b2, z1 = out[0], out[1:3]
            if not s:
                a2 = out[3]

        parts, out = [], ()
        for part in range(2):
            keep, send = ran(incoming(next_step(core), a2, b2, part, 2))
            parts.append((keep, swap(send, 1)))
        for part, (keep, received) in enumerate(parts):
            out = (finish(chip, keep, received, *z1, layer2, part, out),)
        return out[0]

    return jax.shard_map(layers, mesh=mesh,
                         in_specs=(row_spec, mask_spec, P(), P(), P(), P(), P(), P(), P(), P()),
                         out_specs=row_spec, check_vma=False)
```
